128 devices in a mesh: dp: 1, tp: 16 (over z, y), ep: 8 (over x, core).
Axes of the slice: x: 4, y: 4, z: 4, core: 2. Of those that a mesh axis runs over, the one named last changes fastest.
Arguments:
- tokens: bfloat16 [49152, 2048], P(('dp', 'ep', 'tp'))
- expert_ids: int32 [49152, 6], P(('dp', 'ep', 'tp'))
- gates: float32 [49152, 6], P(('dp', 'ep', 'tp'))
- slots: int32 [49152, 6], P(('dp', 'ep', 'tp'))
- shared_w1: bfloat16 [2048, 2816], P(None, 'tp')
- shared_w3: bfloat16 [2048, 2816], P(None, 'tp')
- shared_w2: bfloat16 [2816, 2048], P('tp')
- expert_w1: bfloat16 [64, 2048, 1408], P('ep')
- expert_w3: bfloat16 [64, 2048, 1408], P('ep')
- expert_w2: bfloat16 [64, 1408, 2048], P('ep')
Outputs:
- output: bfloat16 [49152, 2048], P(('dp', 'ep', 'tp'))
All inputs are finite; a program needn't handle non-finite values.
Results may differ from the reference program's by a relative error of at most 0.00146.
Values are sent between devices in bfloat16 or wider.
A program may use at most 1 GiB of HBM per device.

```python
import jax
import jax.numpy as jnp
from jax import lax

D_MODEL = 2048
FF_EXPERT = 1408
FF_SHARED = 2816
EXPERTS = 64
TOP_K = 6
TOKENS_DEV = 384
EP_SIZE = 8
TP_SIZE = 16
CAPACITY = 72

N_SOURCES = EP_SIZE * TP_SIZE
N_TOKENS = N_SOURCES * TOKENS_DEV


def draw_routing(route_key):
    key_hot, key_score = jax.random.split(route_key)
    hot_ids = jax.random.randint(key_hot, (2,), 0, EXPERTS)
    expert_range = jnp.arange(EXPERTS, dtype=jnp.int32)
    scores = jax.random.randint(key_score, (N_TOKENS, EXPERTS), 0, 1024)
    favoured = jnp.any(expert_range[None, :] == hot_ids[:, None], axis=0).astype(jnp.int32) * 128
    row_pos = jnp.arange(N_TOKENS, dtype=jnp.int32) % TOKENS_DEV
    forced = ((row_pos[:, None] < CAPACITY) & (expert_range[None, :] == hot_ids[0])).astype(jnp.int32) * 4096
    keyed_scores = (scores + favoured[None, :] + forced) * EXPERTS + expert_range[None, :]
    top_vals, expert_ids = lax.top_k(keyed_scores, TOP_K)
    expert_ids = expert_ids.astype(jnp.int32)
    per_source = expert_ids.reshape(N_SOURCES, TOKENS_DEV * TOP_K)
    one_hot = (per_source[:, :, None] == expert_range[None, None, :]).astype(jnp.int32)
    position = jnp.sum(jnp.cumsum(one_hot, axis=1) * one_hot, axis=2) - 1
    slots = jnp.where(position < CAPACITY, position, -1)
    return expert_ids, slots.reshape(N_TOKENS, TOP_K).astype(jnp.int32)


def normal_weights(weight_key, shape, fan_in):
    return (jax.random.normal(weight_key, shape, jnp.float32) * fan_in ** -0.5).astype(jnp.bfloat16)


def setup_inputs(seed: int = 0, part: int = 0) -> dict:
    root_key = jax.random.key(seed)
    shared_key, base_key = jax.random.split(root_key)
    part_key = jax.random.fold_in(base_key, part)
    key_tok, key_route, key_gate = jax.random.split(part_key, 3)
    key_list = jax.random.split(shared_key, 6)
    tokens = jax.random.normal(key_tok, (N_TOKENS, D_MODEL), jnp.float32).astype(jnp.bfloat16)
    expert_ids, slots = draw_routing(key_route)
    gates = jax.random.uniform(key_gate, (N_TOKENS, TOP_K), jnp.float32, 0.5, 1.0)
    return {
        "tokens": tokens,
        "expert_ids": expert_ids,
        "gates": gates,
        "slots": slots,
        "shared_w1": normal_weights(key_list[0], (D_MODEL, FF_SHARED), D_MODEL),
        "shared_w3": normal_weights(key_list[1], (D_MODEL, FF_SHARED), D_MODEL),
        "shared_w2": normal_weights(key_list[2], (FF_SHARED, D_MODEL), FF_SHARED),
        "expert_w1": normal_weights(key_list[3], (EXPERTS, D_MODEL, FF_EXPERT), D_MODEL),
        "expert_w3": normal_weights(key_list[4], (EXPERTS, D_MODEL, FF_EXPERT), D_MODEL),
        "expert_w2": normal_weights(key_list[5], (EXPERTS, FF_EXPERT, D_MODEL), FF_EXPERT),
    }


def swiglu_rows(token_rows, w_gate, w_up, w_down):
    gate_pre = jnp.dot(token_rows, w_gate, preferred_element_type=jnp.float32)
    up_pre = jnp.dot(token_rows, w_up, preferred_element_type=jnp.float32)
    hidden = (jax.nn.silu(gate_pre) * up_pre).astype(jnp.bfloat16)
    return jnp.dot(hidden, w_down, preferred_element_type=jnp.float32)


def reference(tokens, expert_ids, gates, slots, shared_w1, shared_w3, shared_w2, expert_w1, expert_w3, expert_w2):
    token_blocks = tokens.reshape(N_SOURCES, TOKENS_DEV, D_MODEL)

    def shared_block(block_rows):
        return swiglu_rows(block_rows, shared_w1, shared_w3, shared_w2)

    shared_out = lax.map(shared_block, token_blocks).reshape(N_TOKENS, D_MODEL)

    tok_ids = jnp.arange(N_TOKENS, dtype=jnp.int32)
    flat_tok = jnp.repeat(tok_ids, TOP_K)
    flat_src = flat_tok // TOKENS_DEV
    flat_exp = expert_ids.reshape(-1)
    flat_slot = jnp.where(slots.reshape(-1) >= 0, slots.reshape(-1), CAPACITY)
    inv_tok = jnp.full((EXPERTS, N_SOURCES, CAPACITY), N_TOKENS, jnp.int32).at[flat_exp, flat_src, flat_slot].set(flat_tok, mode="drop")
    inv_gate = jnp.zeros((EXPERTS, N_SOURCES, CAPACITY), jnp.float32).at[flat_exp, flat_src, flat_slot].set(gates.reshape(-1), mode="drop")

    def expert_step(accum_sum, step_inputs):
        rows_tok, rows_gate, w_gate, w_up, w_down = step_inputs
        tok_flat = rows_tok.reshape(-1)
        token_rows = jnp.take(tokens, tok_flat, axis=0, mode="fill", fill_value=0)
        expert_out = swiglu_rows(token_rows, w_gate, w_up, w_down).astype(jnp.bfloat16)
        weighted = rows_gate.reshape(-1)[:, None] * expert_out.astype(jnp.float32)
        return accum_sum.at[tok_flat].add(weighted, mode="drop"), None

    routed, unused_out = lax.scan(expert_step, jnp.zeros((N_TOKENS, D_MODEL), jnp.float32), (inv_tok, inv_gate, expert_w1, expert_w3, expert_w2))
    y_total = tokens.astype(jnp.float32) + shared_out + routed
    return y_total.astype(jnp.bfloat16)
```

```python
import functools

import jax
import jax.numpy as jnp
from jax import lax
from jax.experimental import pallas as pl
from jax.experimental.pallas import tpu as pltpu
from jax.sharding import PartitionSpec as P

MESH = pl.DeviceIdType.MESH
ANY = pl.BlockSpec(memory_space=pl.ANY)
VM = pl.BlockSpec(memory_space=pltpu.VMEM)
F32 = jnp.float32
BF16 = jnp.bfloat16
DMA = pltpu.SemaphoreType.DMA
VMEM_CAP = 62 * 1024 * 1024
BF16_MAX = 3.3895313892515355e38


def capacity_rows(tok_dev, top_k, n_exp):
    return 8 * max(1, (2 * tok_dev * top_k + 8 * n_exp - 1) // (8 * n_exp))


def nt_dot(a, b):
    return lax.dot_general(a, b, (((1,), (1,)), ((), ())), preferred_element_type=F32)


def peer(k, q, n_ep):
    me = lax.axis_index("ep")
    chips = n_ep // 2
    chip, core = me // 2, lax.rem(me, 2)
    return lax.rem(chip + k, chips) * 2 + lax.rem(core + q, 2)


def meet(others):
    barrier = pltpu.get_barrier_semaphore()
    for other in others:
        pl.semaphore_signal(barrier, inc=1, device_id={"ep": other}, device_id_type=MESH)
    pl.semaphore_wait(barrier, len(others))


def send(src, dst, send_sem, recv_sem, to):
    copy = pltpu.make_async_remote_copy(src_ref=src, dst_ref=dst, send_sem=send_sem, recv_sem=recv_sem, device_id={"ep": to}, device_id_type=MESH)
    copy.start()
    return copy


def gather_kernel(dims, tok, cg, x_out, g_out, sib_out, tokbuf, cgbuf, oh, xst, gst, own_sem, cg_send, cg_recv, ring_send, fwd_send, sib_send, tok_recv, x_sem, g_sem, out_sem):
    n_ep, n_loc, cap, top_k = dims
    t_dev, d_model = tok.shape
    rows = n_loc * cap
    pr = t_dev // 4
    me = lax.axis_index("ep")
    sib = peer(0, 1, n_ep)
    right, left = peer(1, 0, n_ep), peer(3, 0, n_ep)
    own = pltpu.make_async_copy(tok, tokbuf.at[0], own_sem)
    own.start()
    cgbuf[0] = cg[...]
    pending = []
    meet([peer(r // 2, r % 2, n_ep) for r in range(1, n_ep)])

    def piece(r, p):
        return tokbuf.at[r, pl.ds(p * pr, pr), :]

    own.wait()
    for p, q in zip((0, 1, 2, 3), (2, 3, 0, 1)):
        pending.append(send(piece(0, p), piece(6, p), ring_send.at[0, p], tok_recv.at[6, p], right))
        pending.append(send(piece(0, q), piece(2, q), ring_send.at[1, q], tok_recv.at[2, q], left))
        pending.append(send(piece(0, p), piece(1, p), sib_send.at[0, p], tok_recv.at[1, p], sib))
        if p == 0:
            for r in range(1, n_ep):
                k, core = r // 2, r % 2
                back = 2 * ((n_ep // 2 - k) % (n_ep // 2)) + core
                pending.append(send(cg, cgbuf.at[back], cg_send.at[r], cg_recv.at[back], peer(k, core, n_ep)))

    def arrived(r, p):
        pltpu.make_async_copy(piece(r, p), piece(r, p), tok_recv.at[r, p]).wait()

    def relay(r, p):
        arrived(r, p)
        if r == 6 and p < 2:
            pending.append(send(piece(6, p), piece(4, p), fwd_send.at[p], tok_recv.at[4, p], right))
        if r == 2 and p >= 2:
            pending.append(send(piece(2, p), piece(4, p), fwd_send.at[p], tok_recv.at[4, p], left))
        pending.append(send(piece(r, p), piece(r + 1, p), sib_send.at[r // 2, p], tok_recv.at[r + 1, p], sib))

    def codes(r):
        if r:
            pltpu.make_async_copy(cgbuf.at[r], cgbuf.at[r], cg_recv.at[r]).wait()

    base = (me * rows).astype(F32)
    x_copies, g_copies = {}, {}

    def gather(r, slot):
        if slot in x_copies:
            x_copies[slot].wait()
        chunk = 2 * cap

        def one_hot(i, carry):
            place = lax.broadcasted_iota(jnp.int32, (chunk, t_dev), 0) + i * chunk
            want = place.astype(F32) + base
            hit = jnp.zeros((chunk, t_dev), F32)
            for j in range(top_k):
                hit = jnp.where(cgbuf[r, j : j + 1, :] == want, 1.0, hit)
            oh[pl.ds(pl.multiple_of(i * chunk, chunk), chunk), :] = hit.astype(BF16)
            return carry

        lax.fori_loop(0, rows // chunk, one_hot, 0)
        width = 512

        def product(n, carry):
            cols = pl.ds(pl.multiple_of(n * width, width), width)
            xst[slot, :, cols] = jnp.dot(oh[...], tokbuf[r, :, cols], preferred_element_type=F32).astype(BF16)
            return carry

        lax.fori_loop(0, d_model // width, product, 0)
        copy = pltpu.make_async_copy(xst.at[slot], x_out.at[r], x_sem.at[slot])
        copy.start()
        x_copies[slot] = copy

    def gates(r, slot):
        if slot in g_copies:
            g_copies[slot].wait()
        codes(r)
        both = cgbuf[r].T
        chunk = t_dev // 4

        def block(i, carry):
            place = lax.broadcasted_iota(jnp.int32, (chunk, rows), 1).astype(F32) + base
            at = pl.ds(pl.multiple_of(i * chunk, chunk), chunk)
            rows_cg = cgt[at, :]
            full = jnp.zeros((chunk, rows), F32)
            for j in range(top_k):
                full = jnp.where(rows_cg[:, j : j + 1] == place, rows_cg[:, 8 + j : 9 + j], full)
            first = jnp.minimum(full, BF16_MAX).astype(BF16)
            rest = full - first.astype(F32)
            second = rest.astype(BF16)
            third = (rest - second.astype(F32)).astype(BF16)
            gst[slot, at, 0:rows] = first
            gst[slot, at, rows : 2 * rows] = second
            gst[slot, at, 2 * rows : 3 * rows] = third
            return carry

        cgt = xgt
        cgt[...] = both
        lax.fori_loop(0, t_dev // chunk, block, 0)
        copy = pltpu.make_async_copy(gst.at[slot], g_out.at[r], g_sem.at[slot])
        copy.start()
        g_copies[slot] = copy

    xgt = out_sem[1]
    done_sem = out_sem[0]
    gates(0, 0)
    gather(0, 0)
    gates(1, 1)
    for p in range(4):
        arrived(1, p)
    sib_copy = pltpu.make_async_copy(tokbuf.at[1], sib_out, done_sem)
    sib_copy.start()
    gather(1, 1)
    relay(6, 0)
    relay(2, 2)
    gates(2, 0)
    gates(3, 1)
    relay(6, 1)
    relay(2, 3)
    gates(4, 0)
    gates(5, 1)
    gates(6, 0)
    gates(7, 1)
    relay(6, 2)
    relay(2, 0)
    relay(6, 3)
    relay(2, 1)
    gather(6, 0)
    gather(2, 1)
    for p in range(4):
        arrived(7, p)
    gather(7, 0)
    for p in range(4):
        arrived(3, p)
    gather(3, 1)
    for p in (0, 2, 1, 3):
        relay(4, p)
    gather(4, 0)
    for p in range(4):
        arrived(5, p)
    gather(5, 1)
    for copy in list(x_copies.values()) + list(g_copies.values()) + [sib_copy]:
        copy.wait()
    for copy in pending:
        copy.wait_send()


def gather_call(tokens, cg, n_ep, n_loc, cap, top_k):
    t_dev, d_model = tokens.shape
    rows = n_loc * cap

    def kernel(*refs):
        (tok, cgr, x_out, g_out, sib_out, tokbuf, cgbuf, oh, xst, gst, xgt, own_sem, cg_send, cg_recv, ring_send, fwd_send, sib_send, tok_recv, x_sem, g_sem, done_sem) = refs
        gather_kernel((n_ep, n_loc, cap, top_k), tok, cgr, x_out, g_out, sib_out, tokbuf, cgbuf, oh, xst, gst, own_sem, cg_send, cg_recv, ring_send, fwd_send, sib_send, tok_recv, x_sem, g_sem, (done_sem, xgt))

    return pl.pallas_call(
        kernel,
        name="gather_tokens",
        out_shape=(
            jax.ShapeDtypeStruct((n_ep, rows, d_model), BF16),
            jax.ShapeDtypeStruct((n_ep, t_dev, 3 * rows), BF16),
            jax.ShapeDtypeStruct((t_dev, d_model), BF16),
        ),
        in_specs=[ANY, VM],
        out_specs=(ANY, ANY, ANY),
        scratch_shapes=[
            pltpu.VMEM((n_ep, t_dev, d_model), BF16),
            pltpu.VMEM((n_ep, 16, t_dev), F32),
            pltpu.VMEM((rows, t_dev), BF16),
            pltpu.VMEM((2, rows, d_model), BF16),
            pltpu.VMEM((2, t_dev, 3 * rows), BF16),
            pltpu.VMEM((t_dev, 16), F32),
            DMA,
            DMA((n_ep,)),
            DMA((n_ep,)),
            DMA((2, 4)),
            DMA((4,)),
            DMA((4, 4)),
            DMA((n_ep, 4)),
            DMA((2,)),
            DMA((2,)),
            DMA,
        ],
        compiler_params=pltpu.CompilerParams(collective_id=0, has_side_effects=True, vmem_limit_bytes=VMEM_CAP),
    )(tokens, cg)


def hidden_call(x, w1, w3, cap):
    n_ep, rows, d_model = x.shape
    n_loc, _, ff = w1.shape
    m = n_ep * cap

    def kernel(x_ref, w1_ref, w3_ref, h_ref):
        xv = x_ref[...].reshape(m, d_model)
        for at in range(0, ff, 256):
            end = min(at + 256, ff)
            both = jnp.concatenate([w1_ref[:, at:end], w3_ref[:, at:end]], axis=1)
            pre = jnp.dot(xv, both, preferred_element_type=F32)
            h_ref[:, at:end] = (jax.nn.silu(pre[:, : end - at]) * pre[:, end - at :]).astype(BF16)

    return pl.pallas_call(
        kernel,
        name="expert_hidden",
        grid=(n_loc,),
        out_shape=jax.ShapeDtypeStruct((n_loc, m, ff), BF16),
        in_specs=[
            pl.BlockSpec((n_ep, cap, d_model), lambda e: (0, e, 0)),
            pl.BlockSpec((None, d_model, ff), lambda e: (e, 0, 0)),
            pl.BlockSpec((None, d_model, ff), lambda e: (e, 0, 0)),
        ],
        out_specs=pl.BlockSpec((None, m, ff), lambda e: (e, 0, 0)),
        compiler_params=pltpu.CompilerParams(vmem_limit_bytes=VMEM_CAP),
        cost_estimate=pl.CostEstimate(flops=4 * n_loc * m * d_model * ff, bytes_accessed=4 * n_loc * d_model * ff, transcendentals=0),
    )(x, w1, w3)


def combine_call(h, w2, g, hs, w2s, cap):
    n_loc, m, ff = h.shape
    n_ep, t_dev, k3 = g.shape
    d_model = w2.shape[2]
    rows = n_loc * cap
    ffs = hs.shape[1]
    width = 256

    def kernel(h_ref, w2_ref, g_ref, hs_ref, w2s_ref, p_ref, rbuf):
        def down(e, carry):
            r = jnp.dot(h_ref[e], w2_ref[e], preferred_element_type=F32).astype(BF16).astype(F32)
            rbuf[:, pl.ds(pl.multiple_of(e * cap, cap), cap), :] = r.reshape(n_ep, cap, width)
            return carry

        lax.fori_loop(0, n_loc, down, 0)

        def add_up(r, carry):
            rr = rbuf[r].astype(BF16)
            p_ref[r] = jnp.dot(g_ref[r], jnp.concatenate([rr, rr, rr], axis=0), preferred_element_type=F32)
            return carry

        lax.fori_loop(0, n_ep, add_up, 0)
        for q in range(2):
            p_ref[q] += jnp.dot(hs_ref[q * t_dev : (q + 1) * t_dev, :], w2s_ref[...], preferred_element_type=F32)

    once = pl.Buffered(1)
    return pl.pallas_call(
        kernel,
        name="combine",
        grid=(d_model // width,),
        out_shape=jax.ShapeDtypeStruct((d_model // width, n_ep, t_dev, width), F32),
        in_specs=[
            pl.BlockSpec((n_loc, m, ff), lambda b: (0, 0, 0), pipeline_mode=once),
            pl.BlockSpec((n_loc, ff, width), lambda b: (0, 0, b)),
            pl.BlockSpec((n_ep, t_dev, k3), lambda b: (0, 0, 0), pipeline_mode=once),
            pl.BlockSpec((2 * t_dev, ffs), lambda b: (0, 0), pipeline_mode=once),
            pl.BlockSpec((ffs, width), lambda b: (0, b)),
        ],
        out_specs=pl.BlockSpec((None, n_ep, t_dev, width), lambda b: (b, 0, 0, 0)),
        scratch_shapes=[pltpu.VMEM((n_ep, rows, width), F32)],
        compiler_params=pltpu.CompilerParams(vmem_limit_bytes=VMEM_CAP),
        cost_estimate=pl.CostEstimate(flops=2 * n_loc * m * d_model * ff, bytes_accessed=2 * n_loc * d_model * ff, transcendentals=0),
    )(h, w2, g, hs, w2s)


def return_call(parts, tokens, n_ep):
    n_blk, _, t_dev, width = parts.shape
    d_model = tokens.shape[1]
    half = n_blk // 2
    order = [b for pair in zip(range(half), range(half, n_blk)) for b in pair]

    def kernel(p, tok, out, ploc, sibrecv, d2recv, finrecv, ld_sem, sib_send, sib_recv, d2_send, d2_recv, fin_send, fin_recv):
        sib = peer(0, 1, n_ep)
        right, left = peer(1, 0, n_ep), peer(3, 0, n_ep)
        loads = {}
        for b in order:
            for k in (2, 1, 3, 0):
                loads[k, b] = pltpu.make_async_copy(p.at[b, 2 * k], ploc.at[k, b], ld_sem.at[k, b])
        meet([sib, right, left])
        pending = []
        for b in order:
            for k in (2, 1, 3, 0):
                loads[k, b].start()
                pending.append(send(p.at[b, 2 * k + 1], sibrecv.at[k, b], sib_send.at[k, b], sib_recv.at[k, b], sib))

        def merge(k, b):
            loads[k, b].wait()
            pltpu.make_async_copy(sibrecv.at[k, b], sibrecv.at[k, b], sib_recv.at[k, b]).wait()
            ploc[k, b] += sibrecv[k, b]

        def pass_on(b):
            k, to, side = (1, right, 0) if b < half else (3, left, 1)
            pltpu.make_async_copy(d2recv.at[b], d2recv.at[b], d2_recv.at[b]).wait()
            ploc[k, b] += d2recv[b]
            pending.append(send(ploc.at[k, b], finrecv.at[side, b], fin_send.at[side, b], fin_recv.at[side, b], to))

        for i, b in enumerate(order):
            to = right if b < half else left
            merge(2, b)
            pending.append(send(ploc.at[2, b], d2recv.at[b], d2_send.at[b], d2_recv.at[b], to))
            merge(1, b)
            merge(3, b)
            if b < half:
                pending.append(send(ploc.at[3, b], finrecv.at[1, b], fin_send.at[1, b], fin_recv.at[1, b], left))
            else:
                pending.append(send(ploc.at[1, b], finrecv.at[0, b], fin_send.at[0, b], fin_recv.at[0, b], right))
            merge(0, b)
            if i >= 2:
                pass_on(order[i - 2])
        pass_on(order[-2])
        pass_on(order[-1])
        for b in order:
            cols = pl.ds(b * width, width)
            for side in range(2):
                pltpu.make_async_copy(finrecv.at[side, b], finrecv.at[side, b], fin_recv.at[side, b]).wait()
            out[:, cols] = (tok[:, cols].astype(F32) + ploc[0, b] + (finrecv[0, b] + finrecv[1, b])).astype(BF16)
        for copy in pending:
            copy.wait_send()

    return pl.pallas_call(
        kernel,
        name="return_sums",
        out_shape=jax.ShapeDtypeStruct((t_dev, d_model), BF16),
        in_specs=[ANY, VM],
        out_specs=VM,
        scratch_shapes=[
            pltpu.VMEM((4, n_blk, t_dev, width), F32),
            pltpu.VMEM((4, n_blk, t_dev, width), F32),
            pltpu.VMEM((n_blk, t_dev, width), F32),
            pltpu.VMEM((2, n_blk, t_dev, width), F32),
            DMA((4, n_blk)),
            DMA((4, n_blk)),
            DMA((4, n_blk)),
            DMA((n_blk,)),
            DMA((n_blk,)),
            DMA((2, n_blk)),
            DMA((2, n_blk)),
        ],
        compiler_params=pltpu.CompilerParams(collective_id=1, has_side_effects=True, vmem_limit_bytes=VMEM_CAP),
    )(parts, tokens)


def solution(mesh):
    n_ep = mesh.shape["ep"]
    row_spec = P(("dp", "ep", "tp"), None)
    expert_spec = P("ep", None, None)

    def local_layer(tokens, expert_ids, gates, slots, shared_w1, shared_w3, shared_w2, expert_w1, expert_w3, expert_w2):
        t_dev, d_model = tokens.shape
        top_k = expert_ids.shape[1]
        n_loc = expert_w1.shape[0]
        cap = capacity_rows(t_dev, top_k, n_loc * n_ep)
        ffs = shared_w1.shape[1] // 2
        core = lax.rem(lax.axis_index("ep"), 2)

        mine = [lax.dynamic_slice_in_dim(w, core * ffs, ffs, 0) for w in (shared_w1.T, shared_w3.T, shared_w2)]
        ws = lax.all_gather(jnp.concatenate(mine, axis=0), "tp", axis=0, tiled=False)
        w1s, w3s, w2s = (ws[:, i * ffs : (i + 1) * ffs, :].reshape(-1, d_model) for i in range(3))

        code = jnp.where(slots >= 0, expert_ids * cap + slots, -1).astype(F32)
        pad = jnp.zeros((8 - top_k, t_dev), F32)
        cg = jnp.concatenate([code.T, pad - 1.0, gates.T, pad], axis=0)
        x, g, tok_sib = gather_call(tokens, cg, n_ep, n_loc, cap, top_k)
        h = hidden_call(x, expert_w1, expert_w3, cap)
        both = jnp.concatenate([tokens, tok_sib], axis=0)
        hs = (jax.nn.silu(nt_dot(both, w1s)) * nt_dot(both, w3s)).astype(BF16)
        parts = combine_call(h, expert_w2, g, hs, w2s, cap)
        return return_call(parts, tokens, n_ep)

    return jax.shard_map(local_layer, mesh=mesh, in_specs=(row_spec, row_spec, row_spec, row_spec, P(None, "tp"), P(None, "tp"), P("tp", None), expert_spec, expert_spec, expert_spec), out_specs=row_spec, check_vma=False)
```
